32 devices in a mesh: dp: 8 (over z, core), vocab: 4 (over y, x).
Axes of the slice: x: 2, y: 2, z: 4, core: 2. Of those that a mesh axis runs over, the one named last changes fastest.
Arguments:
- hidden: bfloat16 [384, 5120], P('dp')
- head_weight: bfloat16 [32768, 5120], P(('dp', 'vocab'))
- target_ids: int32 [384], P('dp'), may hold values from 0 to 32767
- response_mask: int32 [384], P('dp'), may hold values 0 or 1
- advantages: bfloat16 [384], P('dp'), may hold values from -0.23925781 to 0.23925781
- seq_tokens: int32 [64], P('dp'), may hold values from 24 to 144
- layer_grads: float32 [8, 512, 4096], P('dp', None, 'vocab'), may hold values from -3 to 3
Outputs:
- grad_hidden: bfloat16 [384, 5120], P('dp', 'vocab')
- grad_weight: bfloat16 [32768, 5120], P(('dp', 'vocab'))
- reduced_bucket: float32 [512, 4096], P('dp', 'vocab')
The draws below stay inside these ranges and needn't reach their ends.
All inputs are finite; a program needn't handle non-finite values. No bound on the sum of `response_mask` on one device may be relied on, other than what follows from the above.
Results may differ from the reference program's by a relative error of at most 0.015.
Values may be sent and summed in bfloat16 or wider, within the bound.
A program may use at most 192 MiB of HBM per device.

```python
import math
import jax
import jax.numpy as jnp
from jax import lax

D = 5120
VOC_DEV = 1024
TOK_DEV = 48
BK_COLS = 1024
TOKENS = 384
VOCAB = 32768
SEQS = 64
BK_ROWS = 512
N_DP = 8
N_VOCAB = 4


def head_rows(weight_key, row_ids):

    def single_row(row_index):
        values = jax.random.normal(jax.random.fold_in(weight_key, row_index), (D,), jnp.float32)
        return jnp.clip(values, -6.0, 6.0) * (3.0 / math.sqrt(D))
    return jax.vmap(single_row)(row_ids)


def draw_head_weight(key, part):
    weight_key = jax.random.fold_in(key, 11)
    row_ids = jnp.arange(VOCAB, dtype=jnp.int32).reshape(VOCAB // VOC_DEV, VOC_DEV)
    blocks = lax.map(lambda block_ids: head_rows(weight_key, block_ids).astype(jnp.bfloat16), row_ids)
    return blocks.reshape(VOCAB, D)


def peaked_rows(key, weight_key):
    shard_count = VOCAB // VOC_DEV
    peak_count = min(shard_count, D // 8)
    peak_shards = jnp.arange(peak_count, dtype=jnp.int32) * shard_count // peak_count
    key_offset, key_height = jax.random.split(jax.random.fold_in(key, 31), 2)
    offsets = jax.random.randint(key_offset, (TOKENS, peak_count), 0, VOC_DEV, dtype=jnp.int32)
    peak_ids = peak_shards[None, :] * VOC_DEV + offsets
    heights = 9.0 + jax.random.uniform(key_height, (TOKENS, peak_count), jnp.float32, -1.0, 1.0)

    def one_token(packed):
        peak_rows, peak_height = packed
        head_block = head_rows(weight_key, peak_rows).astype(jnp.bfloat16).astype(jnp.float32)
        gram_matrix = jnp.dot(head_block, head_block.T, precision=lax.Precision.HIGHEST)
        ridge_term = 0.05 * jnp.mean(jnp.diagonal(gram_matrix))
        identity = jnp.eye(peak_count, dtype=jnp.float32)
        coefficients = jnp.linalg.solve(gram_matrix + ridge_term * identity, peak_height)
        return jnp.dot(coefficients, head_block, precision=lax.Precision.HIGHEST)
    return lax.map(one_token, (peak_ids, heights))


def draw_hidden(key, part):
    weight_key = jax.random.fold_in(key, 11)
    hidden_key = jax.random.fold_in(key, 23)
    noise = jnp.clip(jax.random.normal(hidden_key, (TOKENS, D), jnp.float32), -6.0, 6.0)
    values = peaked_rows(key, weight_key) + 0.15 * noise
    values = jnp.clip(values, -6.0, 6.0)
    return values.astype(jnp.bfloat16)


def draw_seq_tokens(key, part):
    position = jnp.arange(SEQS, dtype=jnp.int32)
    centre = TOK_DEV * (SEQS - 1 + 2 * position) // (SEQS - 1)
    key_vals, key_high, key_low = jax.random.split(jax.random.fold_in(key, 37), 3)
    counts = jax.random.randint(key_vals, (SEQS,), centre // 2, centre + 1, dtype=jnp.int32)
    half = SEQS // 2
    high_pos = jax.random.randint(key_high, (), half, SEQS, dtype=jnp.int32)
    low_pos = jax.random.randint(key_low, (), 0, half, dtype=jnp.int32)
    counts = jnp.where(position == high_pos, 3 * TOK_DEV, counts)
    counts = jnp.where(position == low_pos, TOK_DEV // 2, counts)
    return counts.astype(jnp.int32)


def touch_ends(entries, stream_key, smallest, largest):
    spot = [jax.random.randint(jax.random.fold_in(stream_key, axis), (), 0, length) for axis, length in enumerate(entries.shape)]
    widest = entries.shape.index(max(entries.shape))
    next_to = spot[:widest] + [(spot[widest] + 1) % entries.shape[widest]] + spot[widest + 1:]
    return entries.at[tuple(spot)].set(smallest).at[tuple(next_to)].set(largest)


def spiked(values, stream_key, source, target, blocks, factor):
    def block_of(dim):
        return (jnp.arange(values.shape[dim]) // (values.shape[dim] // blocks)).reshape((-1,) + (1,) * (values.ndim - 1 - dim))

    one_side = jax.random.permutation(stream_key, blocks)[block_of(target)]
    far = (block_of(target) + blocks // 2) % blocks
    return jnp.where((block_of(source) == one_side) | (block_of(source) == far), factor * values, values)


def steps_of(key, shape, shards, least, largest):
    level, own = 1.0, jax.random.fold_in(key, 6)
    for dim, shards_of in shards:
        steps = jnp.exp(jax.random.uniform(jax.random.fold_in(own, dim), (shards_of,), jnp.float32, least / len(shards), largest / len(shards)))
        level = level * jnp.repeat(steps, shape[dim] // shards_of).reshape([-1 if axis == dim else 1 for axis in range(len(shape))])
    return level


def gaussian(rng, dims, spread, reach, shards=(), held_as=jnp.bfloat16):
    entries = spread * jax.random.normal(rng, dims, jnp.float32)
    if shards:
        entries = entries * steps_of(rng, dims, shards, -0.22, 0.18)
    return jnp.clip(entries, -reach, reach).astype(held_as)


def noise_with(own_key, dims, spread, reach, cuts, heavy, kind=jnp.bfloat16):
    values = spread * jax.random.normal(own_key, dims, jnp.float32)
    if cuts:
        values = values * steps_of(own_key, dims, cuts, -0.22, 0.18)
    return jnp.clip(spiked(values, jax.random.fold_in(own_key, 3), *heavy), -reach, reach).astype(kind)


def setup_inputs(seed: int = 0) -> dict:
    key_of = jax.random.split(jax.random.key(seed), 8)
    hidden = draw_hidden(jax.random.fold_in(key_of[7], 71), 0)
    head_weight = draw_head_weight(jax.random.fold_in(key_of[7], 71), 0)
    target_ids = touch_ends(jax.random.randint(key_of[2], (TOKENS,), 0, VOCAB), jax.random.fold_in(key_of[2], 1), 0, VOCAB - 1).astype(jnp.int32)
    response_mask = touch_ends((jax.random.randint(key_of[3], (TOKENS,), 0, 4) < 3).astype(jnp.int32), jax.random.fold_in(key_of[3], 1), 0, 1)
    advantages = gaussian(key_of[4], (TOKENS,), 0.04, 0.23925781, ((0, 8),))
    seq_tokens = draw_seq_tokens(jax.random.fold_in(key_of[7], 71), 0)
    layer_grads = noise_with(key_of[6], (N_DP, BK_ROWS, BK_COLS * N_VOCAB), 0.25, 3.0, ((0, 8), (2, 4)), (0, 1, 8, 2.0), jnp.float32)
    return {"hidden": hidden, "head_weight": head_weight, "target_ids": target_ids, "response_mask": response_mask, "advantages": advantages, "seq_tokens": seq_tokens, "layer_grads": layer_grads}


loss_scale = 16.0
entropy_coef = 0.1

def combine_stats(first, second):
    first_max, first_sum, first_ent, first_tgt = first
    second_max, second_sum, second_ent, second_tgt = second
    joint_max = jnp.maximum(first_max, second_max)
    first_f = jnp.exp(first_max - joint_max)
    second_f = jnp.exp(second_max - joint_max)
    return (joint_max, first_sum * first_f + second_sum * second_f, first_ent * first_f + second_ent * second_f, first_tgt + second_tgt)

def reference(hidden, head_weight, target_ids, response_mask, advantages, seq_tokens, layer_grads):
    num_blocks = head_weight.shape[0] // VOC_DEV
    w_blocks = head_weight.reshape(num_blocks, VOC_DEV, D)
    offsets = jnp.arange(num_blocks, dtype=jnp.int32) * VOC_DEV
    local_rows = jnp.arange(VOC_DEV, dtype=jnp.int32)[:, None]

    def logits_of(w_block):
        return jnp.dot(w_block.astype(jnp.float32), hidden.T.astype(jnp.float32), preferred_element_type=jnp.float32)

    def stats_step(running, packed):
        w_block, offset = packed
        logits = logits_of(w_block)
        block_max = jnp.max(logits, axis=0)
        shifted = jnp.exp(logits - block_max[None, :])
        onehot = offset + local_rows == target_ids[None, :]
        block = (block_max, jnp.sum(shifted, axis=0), jnp.sum(shifted * logits, axis=0), jnp.sum(jnp.where(onehot, logits, jnp.zeros_like(logits)), axis=0))
        return (combine_stats(running, block), None)
    tokens = hidden.shape[0]
    start_stats = (jnp.full((tokens,), -jnp.inf, dtype=jnp.float32), jnp.zeros((tokens,), jnp.float32), jnp.zeros((tokens,), jnp.float32), jnp.zeros((tokens,), jnp.float32))
    (row_max, row_sum, row_ent, row_tgt), _ = lax.scan(stats_step, start_stats, (w_blocks, offsets))
    token_total = jnp.sum(seq_tokens.astype(jnp.float32))
    factor = loss_scale * tokens / token_total
    weights = factor * response_mask.astype(jnp.float32)
    advantage = advantages.astype(jnp.float32)
    mean_logit = row_ent / row_sum

    def grad_step(accum, packed):
        w_block, offset = packed
        logits = logits_of(w_block)
        softmax = jnp.exp(logits - row_max[None, :]) / row_sum[None, :]
        onehot = (offset + local_rows == target_ids[None, :]).astype(jnp.float32)
        logit_grad = weights[None, :] * (-advantage[None, :] * (onehot - softmax) + entropy_coef * softmax * (logits - mean_logit[None, :]))
        grad_bf = logit_grad.astype(jnp.bfloat16)
        weight_grad = jnp.dot(grad_bf.astype(jnp.float32), hidden.astype(jnp.float32), preferred_element_type=jnp.float32).astype(jnp.bfloat16)
        accum = accum + jnp.dot(grad_bf.T.astype(jnp.float32), w_block.astype(jnp.float32), preferred_element_type=jnp.float32)
        return (accum, weight_grad)
    grad_sum, weight_grads = lax.scan(grad_step, jnp.zeros((tokens, D), jnp.float32), (w_blocks, offsets))
    grad_hidden = grad_sum.astype(jnp.bfloat16)
    grad_weight = weight_grads.reshape(head_weight.shape[0], D)
    reduced_bucket = jnp.sum(layer_grads, axis=0) * factor
    return (grad_hidden, grad_weight, reduced_bucket)
```

```python
import functools
import jax
import jax.numpy as jnp
from jax import lax
from jax.experimental import pallas as pl
from jax.experimental.pallas import tpu as pltpu
from jax.sharding import PartitionSpec as P

loss_scale = 16.0
entropy_coef = 0.1
MESH = pl.DeviceIdType.MESH
F32 = jnp.float32
BF16 = jnp.bfloat16


def kernel(ndp, nv, hid, w_hbm, meta, lg, hid_out, grad_out, gh_out, bk_out, meta_out,
           w, hall, mbuf, logits, grad_t, gh, st_a, st_b, sa, sb, r1, sbuf, r2, own, t, r3,
           lgb, b1, bs, b2, lsem,
           g1s, g1r, pos, por, ms, mr, b1s, b1r, b2s, b2r, g2s, g2r, hps, hpr,
           sas, sar, sbs, sbr, r1s, r1r, r2s, r2r, r3s, r3r):
    rows, depth = hid.shape
    voc = w.shape[0]
    tokens = hall.shape[0]
    nz = ndp // 2
    quart = depth // nv
    brow = lg.shape[0] // ndp
    dp = lax.axis_index("dp")
    v = lax.axis_index("vocab")
    core = lax.rem(dp, 2)
    z = dp // 2
    mate = 2 * z + 1 - core
    pending = []

    def block(d):
        return pl.ds(pl.multiple_of(d * rows, rows), rows)

    def cols(q):
        return pl.ds(pl.multiple_of(q * quart, quart), quart)

    def bblock(d):
        return pl.ds(pl.multiple_of(d * brow, brow), brow)

    def copy(src, dst, s, r, d, q):
        return pltpu.make_async_remote_copy(
            src_ref=src, dst_ref=dst, send_sem=s, recv_sem=r, device_id=(d, q),
            device_id_type=MESH)

    def send(*args):
        c = copy(*args)
        c.start()
        pending.append(c)

    def arrived(ref, s, r):
        copy(ref, ref, s, r, mate, v).wait_recv()

    def zfwd(k):
        return lax.rem(z + k, nz)

    def zback(k):
        return lax.rem(z + nz - k, nz)

    def vfwd(k):
        return lax.rem(v + k, nv)

    def vback(k):
        return lax.rem(v + nv - k, nv)

    wcopy = pltpu.make_async_copy(w_hbm, w, lsem.at[0])
    wcopy.start()
    barrier = pltpu.get_barrier_semaphore()
    for k in range(1, ndp):
        pl.semaphore_signal(barrier, inc=1, device_id=(lax.rem(dp + k, ndp), v), device_id_type=MESH)
    for k in range(1, nv):
        pl.semaphore_signal(barrier, inc=1, device_id=(dp, vfwd(k)), device_id_type=MESH)
    pl.semaphore_wait(barrier, ndp + nv - 2)

    for k in range(1, nz):
        send(hid.at[:, cols(v)], hall.at[block(dp), cols(v)], g1s.at[k - 1], g1r.at[k - 1],
             2 * zfwd(k) + core, v)
    send(hid, hall.at[block(dp), :], pos.at[0], por.at[0], mate, v)
    for k in range(1, ndp):
        send(meta, mbuf.at[k - 1], ms.at[k - 1], mr.at[k - 1], lax.rem(dp + k, ndp), v)
    hall[block(dp), :] = hid[...]
    lgb[...] = lg[...].astype(BF16)
    for k in range(nz):
        send(lgb.at[bblock(2 * k + 1 - core), :], b1.at[pl.ds(k * brow, brow), :],
             b1s.at[k], b1r.at[k], mate, v)
    for k in range(1, nz):
        ref = hall.at[block(2 * zback(k) + core), cols(v)]
        arrived(ref, g1s.at[k - 1], g1r.at[k - 1])
        for j in range(1, nv):
            i = (k - 1) * (nv - 1) + j - 1
            send(ref, ref, g2s.at[i], g2r.at[i], dp, vfwd(j))
        i = (k - 1) * nv
        send(ref, ref, hps.at[i], hpr.at[i], mate, v)
    for k in range(nz):
        arrived(b1.at[pl.ds(k * brow, brow), :], b1s.at[k], b1r.at[k])
    for k in range(1, nz):
        zz = zfwd(k)
        bs[k - 1] = (lg[bblock(2 * zz + core), :] + b1[bblock(zz), :].astype(F32)).astype(BF16)
        send(bs.at[k - 1], b2.at[k - 1], b2s.at[k - 1], b2r.at[k - 1], 2 * zz + core, v)
    bk_out[...] = lg[bblock(dp), :] + b1[bblock(z), :].astype(F32)
    for k in range(1, ndp):
        arrived(mbuf.at[k - 1], ms.at[k - 1], mr.at[k - 1])
    total = meta[...]
    for k in range(1, ndp):
        total = total + mbuf[k - 1]
    meta_out[...] = total
    for k in range(1, nz):
        for j in range(1, nv):
            i = (k - 1) * (nv - 1) + j - 1
            ref = hall.at[block(2 * zback(k) + core), cols(vback(j))]
            arrived(ref, g2s.at[i], g2r.at[i])
            i = (k - 1) * nv + j
            send(ref, ref, hps.at[i], hpr.at[i], mate, v)
    arrived(hall.at[block(mate), :], pos.at[0], por.at[0])
    for k in range(1, nz):
        for j in range(nv):
            i = (k - 1) * nv + j
            ref = hall.at[block(2 * zback(k) + 1 - core), cols(vback(j))]
            arrived(ref, hps.at[i], hpr.at[i])
    hcopy = pltpu.make_async_copy(hall, hid_out, lsem.at[1])
    hcopy.start()
    wcopy.wait()

    vt = 128

    def logits_step(i, top):
        at = pl.ds(pl.multiple_of(i * vt, vt), vt)
        part = lax.dot_general(w[at, :], hall[...], (((1,), (1,)), ((), ())),
                               preferred_element_type=F32)
        logits[at, :] = part
        return jnp.maximum(top, jnp.max(part, axis=0, keepdims=True))

    top = lax.fori_loop(0, voc // vt, logits_step, jnp.full((1, tokens), -jnp.inf, F32))

    def stats_step(i, carry):
        s, e = carry
        part = logits[pl.ds(pl.multiple_of(i * vt, vt), vt), :]
        x = jnp.exp(part - top)
        return (s + jnp.sum(x, axis=0, keepdims=True), e + jnp.sum(x * part, axis=0, keepdims=True))

    zero = jnp.zeros((1, tokens), F32)
    s, e = lax.fori_loop(0, voc // vt, stats_step, (zero, zero))

    def merge(buf, snd, ss, rs, count, target, m, s, e):
        snd[0:1, :] = m
        snd[1:2, :] = s
        snd[2:3, :] = e
        snd[3:8, :] = jnp.zeros((5, tokens), F32)
        for k in range(1, count):
            send(snd, buf.at[k - 1], ss.at[k - 1], rs.at[k - 1], *target(k))
        for k in range(1, count):
            arrived(buf.at[k - 1], ss.at[k - 1], rs.at[k - 1])
        new = m
        for k in range(1, count):
            new = jnp.maximum(new, buf[k - 1, 0:1, :])
        f = jnp.exp(m - new)
        s, e = s * f, e * f
        for k in range(1, count):
            f = jnp.exp(buf[k - 1, 0:1, :] - new)
            s = s + buf[k - 1, 1:2, :] * f
            e = e + buf[k - 1, 2:3, :] * f
        return new, s, e

    m, s, e = merge(st_a, sa, sas, sar, ndp, lambda k: (lax.rem(dp + k, ndp), v), top, s, e)
    m, s, e = merge(st_b, sb, sbs, sbr, nv, lambda k: (dp, vfwd(k)), m, s, e)

    label = total[0:1, :]
    weight = loss_scale * tokens / total[3:4, :] * total[1:2, :]
    adv = total[2:3, :]
    inv = 1.0 / s
    mean = e * inv
    first = (dp * nv + v) * voc

    def grad_step(i, carry):
        at = pl.ds(pl.multiple_of(i * vt, vt), vt)
        part = logits[at, :]
        p = jnp.exp(part - m) * inv
        ids = (first + i * vt + lax.broadcasted_iota(jnp.int32, part.shape, 0)).astype(F32)
        hot = jnp.where(ids == label, 1.0, 0.0)
        g = weight * (-adv * (hot - p) + entropy_coef * p * (part - mean))
        grad_out[at, :] = g.astype(BF16)
        grad_t[:, at] = g.T.astype(BF16)
        return carry

    lax.fori_loop(0, voc // vt, grad_step, 0)

    ct = 256 if quart % 256 == 0 else 128
    for kq in list(range(1, nv)) + [0]:
        q = vfwd(kq)

        def gh_step(i, carry):
            at = pl.ds(pl.multiple_of(q * quart + i * ct, 128), ct)
            gh[:, at] = jnp.dot(grad_t[...], w[:, at], preferred_element_type=F32).astype(BF16)
            return carry

        lax.fori_loop(0, quart // ct, gh_step, 0)
        for k in range(nz):
            i = kq * nz + k
            zz = zfwd(k)
            send(gh.at[block(2 * zz + 1 - core), cols(q)], r1.at[block(zz), cols(q)],
                 r1s.at[i], r1r.at[i], mate, v)
    for k in list(range(1, nz)) + [0]:
        zz = zfwd(k)
        for kq in list(range(1, nv)) + [0]:
            q = vfwd(kq)
            i = kq * nz + k
            arrived(r1.at[block(zz), cols(q)], r1s.at[i], r1r.at[i])
            both = (gh[block(2 * zz + core), cols(q)].astype(F32)
                    + r1[block(zz), cols(q)].astype(F32))
            if kq:
                i = (kq - 1) * nz + k
                sbuf[i] = both.astype(BF16)
                send(sbuf.at[i], r2.at[i], r2s.at[i], r2r.at[i], dp, q)
            else:
                own[k] = both
    for k in list(range(1, nz)) + [0]:
        acc = own[k]
        for j in range(1, nv):
            i = (j - 1) * nz + k
            arrived(r2.at[i], r2s.at[i], r2r.at[i])
            acc = acc + r2[i].astype(F32)
        if k:
            t[k - 1] = acc.astype(BF16)
            send(t.at[k - 1], r3.at[k - 1], r3s.at[k - 1], r3r.at[k - 1], 2 * zfwd(k) + core, v)
        else:
            own[0] = acc
    bsum = bk_out[...]
    for k in range(1, nz):
        arrived(b2.at[k - 1], b2s.at[k - 1], b2r.at[k - 1])
        bsum = bsum + b2[k - 1].astype(F32)
    bk_out[...] = bsum
    acc = own[0]
    for k in range(1, nz):
        arrived(r3.at[k - 1], r3s.at[k - 1], r3r.at[k - 1])
        acc = acc + r3[k - 1].astype(F32)
    gh_out[...] = acc.astype(BF16)
    hcopy.wait()
    for c in pending:
        c.wait_send()


def on_device(ndp, nv, hidden, head_weight, target_ids, response_mask, advantages, seq_tokens, layer_grads):
    rows, depth = hidden.shape
    voc = head_weight.shape[0]
    tokens = rows * ndp
    nz = ndp // 2
    quart = depth // nv
    bucket = layer_grads[0]
    brows, bcols = bucket.shape
    brow = brows // ndp
    small = jnp.stack([target_ids.astype(F32), response_mask.astype(F32), advantages.astype(F32)])
    meta = lax.dynamic_update_slice(jnp.zeros((8, tokens), F32), small,
                                    (jnp.int32(0), lax.axis_index("dp") * rows))
    meta = meta.at[3].set(jnp.sum(seq_tokens).astype(F32))
    vm = pl.BlockSpec(memory_space=pltpu.VMEM)
    hbm = pl.BlockSpec(memory_space=pl.ANY)
    dma = lambda n: pltpu.SemaphoreType.DMA((n,))
    pairs = [nz - 1, 1, ndp - 1, nz, nz - 1, (nz - 1) * (nv - 1), (nz - 1) * nv,
             ndp - 1, nv - 1, nz * nv, nz * (nv - 1), nz - 1]
    gathered, grad_bf, own_hidden, bucket_sum, total = pl.pallas_call(
        functools.partial(kernel, ndp, nv),
        out_shape=(
            jax.ShapeDtypeStruct((tokens, depth), BF16),
            jax.ShapeDtypeStruct((voc, tokens), BF16),
            jax.ShapeDtypeStruct((rows, quart), BF16),
            jax.ShapeDtypeStruct((brow, bcols), F32),
            jax.ShapeDtypeStruct((8, tokens), F32),
        ),
        in_specs=[vm, hbm, vm, vm],
        out_specs=(hbm, vm, vm, vm, vm),
        scratch_shapes=[
            pltpu.VMEM((voc, depth), BF16),
            pltpu.VMEM((tokens, depth), BF16),
            pltpu.VMEM((ndp - 1, 8, tokens), F32),
            pltpu.VMEM((voc, tokens), F32),
            pltpu.VMEM((tokens, voc), BF16),
            pltpu.VMEM((tokens, depth), BF16),
            pltpu.VMEM((ndp - 1, 8, tokens), F32),
            pltpu.VMEM((nv - 1, 8, tokens), F32),
            pltpu.VMEM((8, tokens), F32),
            pltpu.VMEM((8, tokens), F32),
            pltpu.VMEM((nz * rows, depth), BF16),
            pltpu.VMEM((nz * (nv - 1), rows, quart), BF16),
            pltpu.VMEM((nz * (nv - 1), rows, quart), BF16),
            pltpu.VMEM((nz, rows, quart), F32),
            pltpu.VMEM((nz - 1, rows, quart), BF16),
            pltpu.VMEM((nz - 1, rows, quart), BF16),
            pltpu.VMEM((brows, bcols), BF16),
            pltpu.VMEM((nz * brow, bcols), BF16),
            pltpu.VMEM((nz - 1, brow, bcols), BF16),
            pltpu.VMEM((nz - 1, brow, bcols), BF16),
            pltpu.SemaphoreType.DMA((2,)),
        ] + [dma(n) for n in pairs for _ in range(2)],
        compiler_params=pltpu.CompilerParams(
            collective_id=0, has_side_effects=True, vmem_limit_bytes=67043328),
    )(hidden, head_weight, meta, bucket)
    grad_weight = jnp.dot(grad_bf, gathered, preferred_element_type=F32).astype(BF16)
    factor = loss_scale * tokens / total[3, 0]
    return (own_hidden, grad_weight, bucket_sum * factor)


def solution(mesh):
    in_specs = (
        P("dp", None),
        P(("dp", "vocab"), None),
        P("dp"),
        P("dp"),
        P("dp"),
        P("dp"),
        P("dp", None, "vocab"),
    )
    out_specs = (P("dp", "vocab"), P(("dp", "vocab"), None), P("dp", "vocab"))
    body = functools.partial(on_device, mesh.shape["dp"], mesh.shape["vocab"])
    return jax.shard_map(
        body, mesh=mesh, in_specs=in_specs, out_specs=out_specs, check_vma=False
    )
```
